512 devices in a mesh: orb: 128 (over z, y, core), pair: 4 (over x).
Axes of the slice: x: 4, y: 8, z: 8, core: 2. Of those that a mesh axis runs over, the one named last changes fastest.
Arguments:
- orbitals: float32 [256, 32, 1024], P('orb'), may hold values from -6 to 6
- send_index: int32 [128, 4, 128], P('orb', 'pair'), may hold values from -1 to 1, as said below
- pair_left: int32 [128, 4, 128], P('orb', 'pair'), may hold values from -1 to 1, as said below
- pair_offset: int32 [128, 4, 128], P('orb', 'pair'), may hold values from -8 to 8
Outputs:
- exchange_field: float32 [256, 32, 1024], P('orb', 'pair')
The draws below stay inside these ranges and needn't reach their ends.
Inputs may be any that keep to these rules, and one draw needn't show every extreme that they name: `send_index`: -1 marks an empty route. Toward some orb index, drawn from the seed, every route from every device is live. pair_left[d, p, s + c] is -1 exactly when send_index[s, p, d + c] is -1.
All inputs are finite; a program needn't handle non-finite values.
Results may differ from the reference program's by a relative error of at most 0.0075.
Values may be sent and summed in bfloat16 or wider, within the bound.
No kernel may reach another device: no remote copies, remote signals or barrier semaphores. Data moves between devices by JAX's collectives and lax.ppermute only.
A program may use at most 128 MiB of HBM per device.

```python
import jax
import jax.numpy as jnp
from jax import lax

B = 32
ORB_DEV = 2
CAP = 1
SWEEPS = 2
ORBITALS = 256
N_ORB = 128
N_PAIR = 4


def route_mask(key):
    base = jax.random.fold_in(key, 7)
    level_key, full_key, route_key = jax.random.split(base, 3)
    levels = 2 ** jax.random.randint(level_key, (N_PAIR, N_ORB), 0, 4)
    busiest = jax.random.randint(full_key, (), 0, N_ORB)
    levels = jnp.where(jnp.arange(N_ORB)[None, :] == busiest, 8, levels)
    draws = jax.random.randint(route_key, (N_ORB, N_PAIR, N_ORB, CAP), 0, 8)
    return draws < levels[None, :, :, None]


def draw_send_index(key, part):
    live_mask = route_mask(key)
    chosen = jax.random.randint(jax.random.fold_in(key, 11), (N_ORB, N_PAIR, N_ORB, CAP), 0, ORB_DEV)
    return jnp.where(live_mask, chosen, -1).reshape(N_ORB, N_PAIR, N_ORB * CAP).astype(jnp.int32)


def draw_pair_left(key, part):
    live_mask = jnp.transpose(route_mask(key), (2, 1, 0, 3))
    chosen = jax.random.randint(jax.random.fold_in(key, 13), (N_ORB, N_PAIR, N_ORB, CAP), 0, ORB_DEV)
    return jnp.where(live_mask, chosen, -1).reshape(N_ORB, N_PAIR, N_ORB * CAP).astype(jnp.int32)


def touch_ends(array, key, smallest, high):
    place = [jax.random.randint(jax.random.fold_in(key, axis), (), 0, length) for axis, length in enumerate(array.shape)]
    widest = array.shape.index(max(array.shape))
    next_to = place[:widest] + [(place[widest] + 1) % array.shape[widest]] + place[widest + 1:]
    return array.at[tuple(place)].set(smallest).at[tuple(next_to)].set(high)


def shard_levels(own_key, extent, pieces, smallest, top_value):
    def one(dim, shards_of):
        steps = jax.random.uniform(jax.random.fold_in(jax.random.fold_in(own_key, 6), dim), (shards_of,), jnp.float32, smallest / len(pieces), top_value / len(pieces))
        return jnp.repeat(jnp.exp(steps), extent[dim] // shards_of).reshape((-1,) + (1,) * (len(extent) - dim - 1))

    gain = one(*pieces[0])
    for cut in pieces[1:]:
        gain = gain * one(*cut)
    return gain


def gaussian(stream_key, extent, scale, limit, shards=(), kind=jnp.bfloat16):
    factor_of = shard_levels(stream_key, extent, shards, -0.22, 0.18) if shards else 1.0
    result = jax.random.normal(stream_key, extent, jnp.float32) * scale * factor_of
    return jnp.minimum(jnp.maximum(result, -limit), limit).astype(kind)


def setup_inputs(seed: int = 0) -> dict:
    key_list = jax.random.split(jax.random.key(seed), 5)
    orbitals = gaussian(key_list[0], (ORBITALS, B, B * B), 1.0, 6.0, ((0, 128),), jnp.float32)
    send_index = draw_send_index(jax.random.fold_in(key_list[4], 71), 0)
    pair_left = draw_pair_left(jax.random.fold_in(key_list[4], 71), 0)
    pair_offset = touch_ends(jax.random.randint(key_list[3], (N_ORB, N_PAIR, N_ORB * CAP), -(B // 4), B // 4 + 1), jax.random.fold_in(key_list[3], 1), -(B // 4), (B // 4 + 1) - 1).astype(jnp.int32)
    return dict(orbitals=orbitals, send_index=send_index, pair_left=pair_left, pair_offset=pair_offset)


def neighbours(field):
    box_side = field.shape[1]
    plane = field.shape[2]
    edge_x = jnp.zeros_like(field[:, :1])
    summed = jnp.concatenate([field[:, 1:], edge_x], 1) + jnp.concatenate([edge_x, field[:, :-1]], 1)
    edge_y = jnp.zeros_like(field[:, :, :box_side])
    summed = summed + jnp.concatenate([field[:, :, box_side:], edge_y], 2) + jnp.concatenate([edge_y, field[:, :, :-box_side]], 2)
    edge_z = jnp.zeros_like(field[:, :, :1])
    column = lax.broadcasted_iota(jnp.int32, (1, 1, plane), 2) % box_side
    upper = jnp.where(column < box_side - 1, jnp.concatenate([field[:, :, 1:], edge_z], 2), 0.0)
    lower = jnp.where(column > 0, jnp.concatenate([edge_z, field[:, :, :-1]], 2), 0.0)
    return summed + upper + lower


def pair_work(left, right, offsets):
    box_side = left.shape[1]
    positions = jnp.arange(box_side, dtype=jnp.int32)
    forward = (positions[None, None, :] == positions[None, :, None] - offsets[:, None, None]).astype(jnp.float32)
    shifted_right = jnp.einsum("rxw,rwc->rxc", forward, right.astype(jnp.float32), precision=lax.Precision.HIGHEST)
    left_wide = left.astype(jnp.float32)
    density = left_wide * shifted_right
    potential = jnp.zeros_like(density)
    for sweep_number in range(SWEEPS):
        potential = (neighbours(potential) + density) / 6.0
    to_left = (potential * shifted_right).astype(jnp.bfloat16)
    backward = (positions[None, None, :] == positions[None, :, None] + offsets[:, None, None]).astype(jnp.float32)
    to_right = jnp.einsum("rxw,rwc->rxc", backward, potential * left_wide, precision=lax.Precision.HIGHEST)
    return to_left, to_right.astype(jnp.bfloat16)


def reference(orbitals, send_index, pair_left, pair_offset):
    rounded = orbitals.astype(jnp.bfloat16)
    slot_count = N_ORB * CAP
    source = (jnp.arange(slot_count, dtype=jnp.int32) // CAP).astype(jnp.int32)
    total = jnp.zeros(orbitals.shape, jnp.float32)
    for pair_number in range(N_PAIR):
        def visit(accumulated, owner_index):
            zero = (owner_index * 0).astype(jnp.int32)
            pair_index = (zero + pair_number).astype(jnp.int32)
            left_rows = lax.dynamic_slice(pair_left, (owner_index, pair_index, zero), (1, 1, slot_count)).reshape(slot_count)
            offsets = lax.dynamic_slice(pair_offset, (owner_index, pair_index, zero), (1, 1, slot_count)).reshape(slot_count)
            send_rows = lax.dynamic_slice(send_index, (zero, pair_index, (owner_index * CAP).astype(jnp.int32)), (N_ORB, 1, CAP)).reshape(slot_count)
            live_mask = left_rows >= 0
            left_id = jnp.where(live_mask, owner_index * ORB_DEV + left_rows, 0).astype(jnp.int32)
            right_id = jnp.where(live_mask, source * ORB_DEV + send_rows, 0).astype(jnp.int32)
            left = jnp.where(live_mask[:, None, None], rounded[left_id], jnp.zeros((), jnp.bfloat16))
            right = jnp.where(live_mask[:, None, None], rounded[right_id], jnp.zeros((), jnp.bfloat16))
            to_left, to_right = pair_work(left, right, offsets)
            accumulated = accumulated.at[left_id].add(jnp.where(live_mask[:, None, None], to_left.astype(jnp.float32), 0.0))
            accumulated = accumulated.at[right_id].add(jnp.where(live_mask[:, None, None], to_right.astype(jnp.float32), 0.0))
            return accumulated, None

        start = jnp.zeros(orbitals.shape, jnp.float32)
        partial_value, unused = lax.scan(visit, start, jnp.arange(N_ORB, dtype=jnp.int32))
        partial_rounded = lax.optimization_barrier(partial_value.astype(jnp.bfloat16))
        total = total + partial_rounded.astype(jnp.float32)
    return -0.25 * total
```

```python
import jax
import jax.numpy as jnp
from jax import lax
from jax.experimental import pallas as pl
from jax.experimental.pallas import tpu as pltpu
from jax.sharding import PartitionSpec as P

PAD = 8
UNROLL = 4


def exchange_kernel(box, planes, unroll):
    side = box
    stride = 2 * side + 3 * PAD + 1

    def kernel(owner_ref, where_ref, own_ref, boxes_hbm, out_ref, boxes, corr, lists, sem):
        peers = boxes_hbm.shape[0]
        tasks = owner_ref.shape[0]
        copies = [
            pltpu.make_async_copy(
                boxes_hbm.at[:, pl.ds(k * side, side)],
                boxes.at[pl.ds(0, peers), pl.ds(PAD + k * (side + PAD), side)],
                sem.at[k],
            )
            for k in range(2)
        ]
        for copy in copies:
            copy.start()

        zero = jnp.zeros((PAD, 8, 128), jnp.bfloat16)

        def clear(q, _):
            boxes[q, pl.ds(0, PAD)] = zero
            boxes[q, pl.ds(PAD + side, PAD)] = zero
            boxes[q, pl.ds(2 * PAD + 2 * side, PAD)] = zero
            boxes[q, 3 * PAD + 2 * side] = zero[0]
            return 0

        lax.fori_loop(0, peers, clear, 0)
        for x in range(stride):
            boxes[peers, x] = zero[0]
        corr[...] = jnp.zeros(corr.shape, corr.dtype)

        def append(k, counts):
            owner = owner_ref[k]
            code = where_ref[k]
            lists[0, counts[0]] = code
            lists[1, counts[1]] = code
            return (
                counts[0] + (owner == 0).astype(jnp.int32),
                counts[1] + (owner == 1).astype(jnp.int32),
            )

        counts = lax.fori_loop(0, tasks, append, (jnp.int32(0), jnp.int32(0)))
        for a in range(2):
            for u in range(unroll):
                lists[a, counts[a] + u] = peers * 128
        for copy in copies:
            copy.wait()

        lane = lax.broadcasted_iota(jnp.int32, (8, 128), 1)
        row = lax.broadcasted_iota(jnp.int32, (8, 128), 0)

        def up_y(value):
            turned = pltpu.roll(value, 96, 1)
            return jnp.where(lane < 96, turned, pltpu.roll(turned, 7, 0))

        def down_y(value):
            turned = pltpu.roll(value, 32, 1)
            return jnp.where(lane >= 32, turned, pltpu.roll(turned, 1, 0))

        def owned(a, _):
            count = jnp.where(a == 0, counts[0], counts[1])

            def group(g, _):
                at = []
                for u in range(unroll):
                    code = lists[a, g * unroll + u]
                    at.append((code >> 7, code & 127))

                def plane(u, x):
                    return boxes[at[u][0], at[u][1] + x].astype(jnp.float32)

                current = [plane(u, 0) for u in range(unroll)]
                for x in range(side):
                    following = [plane(u, x + 1) for u in range(unroll)]
                    sums = [corr[a, k, x] for k in range(4)]
                    for u in range(unroll):
                        value = current[u]
                        sums[0] = sums[0] + value * value
                        sums[1] = sums[1] + value * following[u]
                        sums[2] = sums[2] + value * up_y(value)
                        sums[3] = sums[3] + value * pltpu.roll(value, 127, 1)
                    for k in range(4):
                        corr[a, k, x] = sums[k]
                    current = following
                return 0

            lax.fori_loop(0, (count + unroll - 1) // unroll, group, 0)
            return 0

        lax.fori_loop(0, 2, owned, 0)

        keep_y = jnp.logical_not(jnp.logical_and(lane >= 96, row == 7))
        keep_z = (lane % 32) < 31

        def finish(a, _):
            before = None
            for x in range(side):
                value = own_ref[a * side + x].astype(jnp.float32)
                self_part = value * corr[a, 0, x]
                along_y = jnp.where(keep_y, corr[a, 2, x], 0.0)
                along_z = jnp.where(keep_z, corr[a, 3, x], 0.0)
                total = (
                    up_y(value) * along_y
                    + down_y(value * along_y)
                    + pltpu.roll(value, 127, 1) * along_z
                    + pltpu.roll(value * along_z, 1, 1)
                )
                if x > 0:
                    total = total + before
                if x < side - 1:
                    along_x = corr[a, 1, x]
                    total = total + own_ref[a * side + x + 1].astype(jnp.float32) * along_x
                    before = value * along_x
                out_ref[a, x] = ((self_part + total / 6.0) / 6.0).astype(out_ref.dtype)
            return 0

        lax.fori_loop(0, 2, finish, 0)

    return kernel, stride


def apply_exchange(owner, where, own, boxes, interpret=False):
    peers = boxes.shape[0]
    side = own.shape[0] // 2
    kernel, stride = exchange_kernel(side, own.shape[0], UNROLL)
    tasks = owner.shape[0]
    return pl.pallas_call(
        kernel,
        out_shape=jax.ShapeDtypeStruct((2, side, 8, 128), jnp.bfloat16),
        in_specs=[
            pl.BlockSpec(memory_space=pltpu.SMEM),
            pl.BlockSpec(memory_space=pltpu.SMEM),
            pl.BlockSpec(memory_space=pltpu.VMEM),
            pl.BlockSpec(memory_space=pl.ANY),
        ],
        out_specs=pl.BlockSpec(memory_space=pltpu.VMEM),
        scratch_shapes=[
            pltpu.VMEM((peers + 1, stride, 8, 128), jnp.bfloat16),
            pltpu.VMEM((2, 4, side, 8, 128), jnp.float32),
            pltpu.SMEM((2, tasks + UNROLL), jnp.int32),
            pltpu.SemaphoreType.DMA((2,)),
        ],
        compiler_params=pltpu.CompilerParams(vmem_limit_bytes=40 * 1024 * 1024),
        interpret=interpret,
    )(owner, where, own, boxes)


def tasks_of(send_rows, left_rows, offsets, send_in, left_in, offset_in, side):
    peer = jnp.arange(send_rows.shape[0], dtype=jnp.int32) * 128 + PAD
    step = side + PAD
    as_left = peer + send_in * step - offsets
    as_right = peer + left_in * step + offset_in
    owner = jnp.concatenate([left_rows, send_rows])
    where = jnp.concatenate([as_left, as_right])
    return owner, where


def local(orbitals, send_index, pair_left, pair_offset):
    owned, side, width = orbitals.shape
    send_rows = send_index.reshape(-1)
    left_rows = pair_left.reshape(-1)
    offsets = pair_offset.reshape(-1)
    peers = send_rows.shape[0]
    own = orbitals.astype(jnp.bfloat16).reshape(owned * side, width // 128, 128)
    meta = jnp.stack([send_rows, left_rows, offsets]).astype(jnp.bfloat16)
    meta = jnp.pad(meta, ((0, 5), (0, 0)))[None]
    payload = jnp.concatenate([own, meta], 0)
    gathered = lax.all_gather(payload, "orb", axis=0, tiled=False)
    me = lax.axis_index("orb")
    column = lax.dynamic_slice(gathered, (0, owned * side, 0, me), (peers, 1, 8, 1))
    column = column.reshape(peers, 8)[:, :3].astype(jnp.int32)
    owner, where = tasks_of(
        send_rows, left_rows, offsets, column[:, 0], column[:, 1], column[:, 2], side
    )
    partial = apply_exchange(owner, where, own, gathered)
    n_pair = lax.axis_size("pair")
    pieces = partial.reshape(owned, n_pair, side // n_pair, width // 128, 128)
    pieces = lax.all_to_all(jnp.moveaxis(pieces, 1, 0), "pair", 0, 0, tiled=True)
    field = -0.25 * jnp.sum(pieces.astype(jnp.float32), axis=0)
    return field.reshape(owned, side // n_pair, width)


def solution(mesh):
    return jax.shard_map(
        local,
        mesh=mesh,
        in_specs=(
            P("orb", None, None),
            P("orb", "pair", None),
            P("orb", "pair", None),
            P("orb", "pair", None),
        ),
        out_specs=P("orb", "pair", None),
        check_vma=False,
    )
```

```python
import jax
import jax.numpy as jnp
import numpy as np
from jax import lax
from jax.experimental import pallas as pl
from jax.experimental.pallas import tpu as pltpu
from jax.sharding import Mesh, PartitionSpec as P

FIELDS = 4
PAD = 8
UNROLL = 4
OWNER_BIT = 20


def tile_kernel(side):
    blocks = side // 8
    pitch = side + PAD
    reach = FIELDS * pitch

    def kernel(count_ref, code_ref, own_ref, peer_ref, out_ref, pairs):
        lane = lax.broadcasted_iota(jnp.int32, (8, 128), 1)
        row = lax.broadcasted_iota(jnp.int32, (8, 128), 0)
        zero = jnp.zeros((8, 128), jnp.float32)
        keep_z = (lane % 32) < 31

        def boxes(ref, peer, a):
            here = [
                ref[peer, pl.ds(a * side + 8 * j, 8)].astype(jnp.float32) for j in range(blocks)
            ]
            edge = ref[peer, pl.ds(2 * side + 8 * a, 8)].astype(jnp.float32)
            turned = [pltpu.roll(v, 7, 0) for v in here] + [zero]
            up_x = [jnp.where(row < 7, turned[j], turned[j + 1]) for j in range(blocks)]
            up_y = []
            for j in range(blocks):
                shift = (96 - 32 * j) % 128
                beyond = pltpu.roll(edge, shift, 1) if shift else edge
                up_y.append(jnp.where(lane < 96, pltpu.roll(here[j], 96, 1), beyond))
            up_z = [pltpu.roll(v, 127, 1) for v in here]
            return here, up_x, up_y, up_z

        def build(peer, _):
            for a in range(2):
                here, up_x, up_y, up_z = boxes(peer_ref, peer, a)
                base = pl.multiple_of((peer * 2 + a) * reach, 8)
                for k, other in enumerate((here, up_x, up_y, up_z)):
                    pairs[pl.ds(base + k * pitch, 8)] = zero
                    for j in range(blocks):
                        pairs[pl.ds(base + k * pitch + PAD + 8 * j, 8)] = here[j] * other[j]
            return 0

        peers = peer_ref.shape[0]
        lax.fori_loop(0, peers, build, 0)
        pairs[pl.ds(peers * 2 * reach, PAD)] = zero

        def finish(own, _):
            edges = []
            for a in range(2):
                first = count_ref[own, 0] if a else jnp.int32(0)
                count = count_ref[own, a]

                def add(index, sums):
                    start = code_ref[own, index] & ((1 << OWNER_BIT) - 1)
                    return [
                        sums[k * blocks + j] + pairs[pl.ds(start + k * pitch + 8 * j, 8)]
                        for k in range(FIELDS)
                        for j in range(blocks)
                    ]

                def several(g, sums):
                    for u in range(UNROLL):
                        sums = add(first + g * UNROLL + u, sums)
                    return sums

                groups = count // UNROLL
                sums = [zero] * (FIELDS * blocks)
                sums = lax.fori_loop(0, groups, several, sums)
                sums = lax.fori_loop(
                    first + groups * UNROLL, first + count, lambda i, s: add(i, s), sums
                )
                here, up_x, up_y, up_z = boxes(own_ref, own, a)
                before = zero
                for j in range(blocks):
                    self_sum, along_x, along_y, along_z = [
                        sums[k * blocks + j] for k in range(FIELDS)
                    ]
                    along_z = jnp.where(keep_z, along_z, 0.0)
                    back_x = pltpu.roll(here[j] * along_x, 1, 0)
                    back_y = here[j] * along_y
                    back_z = pltpu.roll(here[j] * along_z, 1, 1)
                    total = up_x[j] * along_x + jnp.where(row > 0, back_x, before)
                    total = total + up_y[j] * along_y
                    total = total + jnp.where(lane >= 32, pltpu.roll(back_y, 32, 1), 0.0)
                    total = total + (up_z[j] * along_z + back_z)
                    before = back_x
                    total = (here[j] * self_sum + total / 6.0) / 6.0
                    chunk = own * blocks + j
                    out_ref[chunk, pl.ds(8 * a, 8)] = total.astype(out_ref.dtype)
                    past = pltpu.roll(back_y, 32 + 32 * a, 1) / 36.0
                    if a == 0:
                        edges.append(past)
                    else:
                        both = jnp.where(lane < 32, edges[j], past)
                        out_ref[chunk, pl.ds(16, 8)] = both.astype(out_ref.dtype)
            return 0

        lax.fori_loop(0, own_ref.shape[0], finish, 0)

    return kernel


def apply_tile(counts, codes, own, peer, side, interpret=False):
    blocks = side // 8
    rows = peer.shape[0] * 2 * FIELDS * (side + PAD) + PAD
    smem = pl.BlockSpec(memory_space=pltpu.SMEM)
    vmem = pl.BlockSpec(memory_space=pltpu.VMEM)
    return pl.pallas_call(
        tile_kernel(side),
        out_shape=jax.ShapeDtypeStruct((own.shape[0] * blocks, 24, 128), jnp.bfloat16),
        in_specs=[smem, smem, vmem, vmem],
        out_specs=vmem,
        scratch_shapes=[pltpu.VMEM((rows, 128), jnp.float32)],
        compiler_params=pltpu.CompilerParams(vmem_limit_bytes=16 * 1024 * 1024),
        interpret=interpret,
    )(counts, codes, own, peer)


def tasks_of(own_meta, peer_meta, side):
    reach = FIELDS * (side + PAD)
    peers = own_meta.shape[2]
    base = jnp.arange(peers, dtype=jnp.int32)[None, :, None] * 2

    def keys(owner, partner, back):
        start = (base + partner) * reach + PAD - back
        return jnp.where(owner >= 0, (owner << OWNER_BIT) + start, 4 << OWNER_BIT)

    as_left = keys(own_meta[1], peer_meta[0], own_meta[2])
    as_right = keys(own_meta[0], peer_meta[1], -peer_meta[2])
    owners = jnp.concatenate([own_meta[1], own_meta[0]], 1).reshape(own_meta.shape[1], -1)
    codes = jnp.concatenate([as_left, as_right], 1).reshape(own_meta.shape[1], -1)
    counts = jnp.stack([jnp.sum(owners == a, 1, dtype=jnp.int32) for a in range(2)], 1)
    return counts, lax.sort(codes, dimension=1, is_stable=False)


def payload_of(rounded, meta, slab):
    owned, side, width = rounded.shape
    wide = jnp.pad(rounded, ((0, 0), (0, 0), (0, 128)))
    part = lax.dynamic_slice(wide, (0, 0, slab * 128), (owned, side, 128 + side))
    edge = part[:, :, 128:].reshape(owned, side // 8, 8, side)
    edge = jnp.moveaxis(edge, 1, 2).reshape(owned * 8, 128)
    return jnp.concatenate([part[:, :, :128].reshape(owned * side, 128), edge, meta], 0)


def meta_of(received, kinds, pairs):
    meta = received[:, 80 : 80 + kinds * pairs].astype(jnp.int32)
    return meta.reshape(received.shape[0], pairs, kinds, 128)


def local(orbitals, send_index, pair_left, pair_offset):
    owned, side, width = orbitals.shape
    pairs = lax.axis_size("x")
    cores = lax.axis_size("c")
    z_size = lax.axis_size("z")
    y_size = lax.axis_size("y")
    x = lax.axis_index("x")
    y = lax.axis_index("y")
    z = lax.axis_index("z")
    rounded = orbitals.astype(jnp.bfloat16)
    meta = jnp.stack([send_index.reshape(-1), pair_left.reshape(-1), pair_offset.reshape(-1)])
    meta = jnp.broadcast_to(meta.astype(jnp.bfloat16)[None], (pairs, 3, 128))
    meta = lax.all_to_all(meta, "x", 0, 0, tiled=True).reshape(pairs * 3, 128)
    meta = jnp.pad(meta, ((0, 4), (0, 0)))
    payload = jnp.stack([payload_of(rounded, meta, c * pairs + x) for c in range(cores)])
    to_peers = jnp.broadcast_to(payload[None], (y_size,) + payload.shape)
    to_peers = to_peers.reshape((y_size * cores,) + payload.shape[1:])
    own = lax.all_to_all(to_peers, ("z", "c"), 0, 0, tiled=True)
    peer = lax.all_to_all(to_peers, ("y", "c"), 0, 0, tiled=True)

    own_meta = meta_of(own, 3, pairs)
    own_meta = lax.dynamic_slice_in_dim(own_meta, z * (y_size * cores), y_size * cores, 3)
    own_meta = jnp.transpose(own_meta, (2, 0, 3, 1))
    peer_meta = meta_of(peer, 3, pairs).reshape(-1, pairs, 3, z_size, y_size, cores)
    peer_meta = lax.dynamic_index_in_dim(peer_meta, y, 4, keepdims=False)
    peer_meta = peer_meta.reshape(-1, pairs, 3, z_size * cores)
    peer_meta = jnp.transpose(peer_meta, (2, 3, 0, 1))
    counts, codes = tasks_of(own_meta, peer_meta, side)

    partial = apply_tile(counts, codes, own, peer, side)
    landed = lax.all_to_all(partial, ("z", "c", "x"), 0, 0, tiled=True)
    landed = landed.reshape(z_size, cores * pairs, 24, 128).astype(jnp.float32)
    slabs = jnp.sum(landed, 0)
    field = slabs[:, :16].reshape(cores * pairs, owned, 8, 128)
    edge = slabs[:-1, 16:, : owned * 32].reshape(-1, 8, owned, 32)
    edge = jnp.moveaxis(edge, 2, 1)
    field = field + jnp.pad(edge, ((1, 0), (0, 0), (0, 0), (0, 96)))
    field = -0.25 * field
    return jnp.transpose(field, (1, 2, 0, 3)).reshape(owned, 8, width)


def solution(mesh):
    fine = Mesh(np.asarray(mesh.devices).reshape(8, 8, 2, 4), ("z", "y", "c", "x"))
    orb = ("z", "y", "c")
    return jax.shard_map(
        local,
        mesh=fine,
        in_specs=(
            P(orb, None, None),
            P(orb, "x", None),
            P(orb, "x", None),
            P(orb, "x", None),
        ),
        out_specs=P(orb, "x", None),
        check_vma=False,
    )
```

```python
import jax
import jax.numpy as jnp
import numpy as np
from jax import lax
from jax.experimental import pallas as pl
from jax.experimental.pallas import tpu as pltpu
from jax.sharding import Mesh, PartitionSpec as P

FIELDS = 4
PAD = 8
UNROLL = 4
OWNER_BIT = 20
ENTRY_BITS = 7


def tile_kernel(side):
    blocks = side // 8
    pitch = side + PAD
    reach = FIELDS * pitch

    def kernel(count_ref, code_ref, own_ref, peer_ref, out_ref, pairs):
        lane = lax.broadcasted_iota(jnp.int32, (8, 128), 1)
        row = lax.broadcasted_iota(jnp.int32, (8, 128), 0)
        zero = jnp.zeros((8, 128), jnp.float32)
        keep_z = (lane % 32) < 31

        def boxes(ref, peer, a):
            here = [
                ref[peer, pl.ds(a * side + 8 * j, 8)].astype(jnp.float32) for j in range(blocks)
            ]
            edge = ref[peer, pl.ds(2 * side + 8 * a, 8)].astype(jnp.float32)
            turned = [pltpu.roll(v, 7, 0) for v in here] + [zero]
            up_x = [jnp.where(row < 7, turned[j], turned[j + 1]) for j in range(blocks)]
            up_y = []
            for j in range(blocks):
                shift = (96 - 32 * j) % 128
                beyond = pltpu.roll(edge, shift, 1) if shift else edge
                up_y.append(jnp.where(lane < 96, pltpu.roll(here[j], 96, 1), beyond))
            up_z = [pltpu.roll(v, 127, 1) for v in here]
            return here, up_x, up_y, up_z

        def build(peer, _):
            for a in range(2):
                here, up_x, up_y, up_z = boxes(peer_ref, peer, a)
                base = pl.multiple_of((peer * 2 + a) * reach, 8)
                for k, other in enumerate((here, up_x, up_y, up_z)):
                    pairs[pl.ds(base + k * pitch, 8)] = zero
                    for j in range(blocks):
                        pairs[pl.ds(base + k * pitch + PAD + 8 * j, 8)] = here[j] * other[j]
            return 0

        peers = peer_ref.shape[0]
        lax.fori_loop(0, peers, build, 0)
        pairs[pl.ds(peers * 2 * reach, PAD)] = zero

        def finish(own, _):
            edges = []
            for a in range(2):
                first = count_ref[own, 0] if a else jnp.int32(0)
                count = count_ref[own, a]

                def add(index, sums):
                    start = (code_ref[own, index] & ((1 << OWNER_BIT) - 1)) >> ENTRY_BITS
                    return [
                        sums[k * blocks + j] + pairs[pl.ds(start + k * pitch + 8 * j, 8)]
                        for k in range(FIELDS)
                        for j in range(blocks)
                    ]

                def several(g, sums):
                    for u in range(UNROLL):
                        sums = add(first + g * UNROLL + u, sums)
                    return sums

                groups = count // UNROLL
                sums = [zero] * (FIELDS * blocks)
                sums = lax.fori_loop(0, groups, several, sums)
                sums = lax.fori_loop(
                    first + groups * UNROLL, first + count, lambda i, s: add(i, s), sums
                )
                here, up_x, up_y, up_z = boxes(own_ref, own, a)
                before = zero
                for j in range(blocks):
                    self_sum, along_x, along_y, along_z = [
                        sums[k * blocks + j] for k in range(FIELDS)
                    ]
                    along_z = jnp.where(keep_z, along_z, 0.0)
                    back_x = pltpu.roll(here[j] * along_x, 1, 0)
                    back_y = here[j] * along_y
                    back_z = pltpu.roll(here[j] * along_z, 1, 1)
                    total = up_x[j] * along_x + jnp.where(row > 0, back_x, before)
                    total = total + up_y[j] * along_y
                    total = total + jnp.where(lane >= 32, pltpu.roll(back_y, 32, 1), 0.0)
                    total = total + (up_z[j] * along_z + back_z)
                    before = back_x
                    total = (here[j] * self_sum + total / 6.0) / 6.0
                    chunk = own * blocks + j
                    out_ref[chunk, pl.ds(8 * a, 8)] = total.astype(out_ref.dtype)
                    past = pltpu.roll(back_y, 32 + 32 * a, 1) / 36.0
                    if a == 0:
                        edges.append(past)
                    else:
                        both = jnp.where(lane < 32, edges[j], past)
                        out_ref[chunk, pl.ds(16, 8)] = both.astype(out_ref.dtype)
            return 0

        lax.fori_loop(0, own_ref.shape[0], finish, 0)

    return kernel


def apply_tile(counts, codes, own, peer, side, interpret=False):
    blocks = side // 8
    rows = peer.shape[0] * 2 * FIELDS * (side + PAD) + PAD
    smem = pl.BlockSpec(memory_space=pltpu.SMEM)
    vmem = pl.BlockSpec(memory_space=pltpu.VMEM)
    return pl.pallas_call(
        tile_kernel(side),
        out_shape=jax.ShapeDtypeStruct((own.shape[0] * blocks, 24, 128), jnp.bfloat16),
        in_specs=[smem, smem, vmem, vmem],
        out_specs=vmem,
        scratch_shapes=[pltpu.VMEM((rows, 128), jnp.float32)],
        compiler_params=pltpu.CompilerParams(vmem_limit_bytes=16 * 1024 * 1024),
        interpret=interpret,
    )(counts, codes, own, peer)


def tasks_of(own_meta, peer_meta, side):
    reach = FIELDS * (side + PAD)
    peers = own_meta.shape[2]
    base = jnp.arange(peers, dtype=jnp.int32)[None, :, None] * 2

    def keys(owner, partner, back):
        start = (base + partner) * reach + PAD - back
        return jnp.where(owner >= 0, (owner << OWNER_BIT) + (start << ENTRY_BITS), 4 << OWNER_BIT)

    as_left = keys(own_meta[1], peer_meta[0], own_meta[2])
    as_right = keys(own_meta[0], peer_meta[1], -peer_meta[2])
    owners = jnp.concatenate([own_meta[1], own_meta[0]], 1).reshape(own_meta.shape[1], -1)
    codes = jnp.concatenate([as_left, as_right], 1).reshape(own_meta.shape[1], -1)
    codes = codes + jnp.arange(codes.shape[1], dtype=jnp.int32)
    counts = jnp.stack([jnp.sum(owners == a, 1, dtype=jnp.int32) for a in range(2)], 1)
    rank = jnp.sum(codes[:, None, :] < codes[:, :, None], 2, dtype=jnp.int32)
    slot = jnp.arange(codes.shape[1], dtype=jnp.int32)
    placed = jnp.where(rank[:, None, :] == slot[None, :, None], codes[:, None, :], 0)
    return counts, jnp.sum(placed, 2, dtype=jnp.int32)


def payload_of(rounded, meta, slab):
    owned, side, width = rounded.shape
    wide = jnp.pad(rounded, ((0, 0), (0, 0), (0, 128)))
    part = lax.dynamic_slice(wide, (0, 0, slab * 128), (owned, side, 128 + side))
    edge = part[:, :, 128:].reshape(owned, side // 8, 8, side)
    edge = jnp.moveaxis(edge, 1, 2).reshape(owned * 8, 128)
    return jnp.concatenate([part[:, :, :128].reshape(owned * side, 128), edge, meta], 0)


def meta_of(received, kinds, pairs):
    meta = received[:, 80 : 80 + kinds * pairs].astype(jnp.int32)
    return meta.reshape(received.shape[0], pairs, kinds, 128)


def local(orbitals, send_index, pair_left, pair_offset):
    owned, side, width = orbitals.shape
    pairs = lax.axis_size("x")
    cores = lax.axis_size("c")
    z_size = lax.axis_size("z")
    y_size = lax.axis_size("y")
    x = lax.axis_index("x")
    y = lax.axis_index("y")
    z = lax.axis_index("z")
    rounded = orbitals.astype(jnp.bfloat16)
    meta = jnp.stack([send_index.reshape(-1), pair_left.reshape(-1), pair_offset.reshape(-1)])
    meta = jnp.broadcast_to(meta.astype(jnp.bfloat16)[None], (pairs, 3, 128))
    meta = lax.all_to_all(meta, "x", 0, 0, tiled=True).reshape(pairs * 3, 128)
    meta = jnp.pad(meta, ((0, 4), (0, 0)))
    payload = jnp.stack([payload_of(rounded, meta, c * pairs + x) for c in range(cores)])
    to_peers = jnp.broadcast_to(payload[None], (y_size,) + payload.shape)
    to_peers = to_peers.reshape((y_size * cores,) + payload.shape[1:])
    own = lax.all_to_all(to_peers, ("z", "c"), 0, 0, tiled=True)
    peer = lax.all_to_all(to_peers, ("y", "c"), 0, 0, tiled=True)

    own_meta = meta_of(own, 3, pairs)
    own_meta = lax.dynamic_slice_in_dim(own_meta, z * (y_size * cores), y_size * cores, 3)
    own_meta = jnp.transpose(own_meta, (2, 0, 3, 1))
    peer_meta = meta_of(peer, 3, pairs).reshape(-1, pairs, 3, z_size, y_size, cores)
    peer_meta = lax.dynamic_index_in_dim(peer_meta, y, 4, keepdims=False)
    peer_meta = peer_meta.reshape(-1, pairs, 3, z_size * cores)
    peer_meta = jnp.transpose(peer_meta, (2, 3, 0, 1))
    counts, codes = tasks_of(own_meta, peer_meta, side)

    partial = apply_tile(counts, codes, own, peer, side)
    landed = lax.all_to_all(partial, ("z", "c", "x"), 0, 0, tiled=True)
    landed = landed.reshape(z_size, cores * pairs, 24, 128).astype(jnp.float32)
    slabs = jnp.sum(landed, 0)
    field = slabs[:, :16].reshape(cores * pairs, owned, 8, 128)
    edge = slabs[:-1, 16:, : owned * 32].reshape(-1, 8, owned, 32)
    edge = jnp.moveaxis(edge, 2, 1)
    field = field + jnp.pad(edge, ((1, 0), (0, 0), (0, 0), (0, 96)))
    field = -0.25 * field
    return jnp.transpose(field, (1, 2, 0, 3)).reshape(owned, 8, width)


def solution(mesh):
    fine = Mesh(np.asarray(mesh.devices).reshape(8, 8, 2, 4), ("z", "y", "c", "x"))
    orb = ("z", "y", "c")
    return jax.shard_map(
        local,
        mesh=fine,
        in_specs=(
            P(orb, None, None),
            P(orb, "x", None),
            P(orb, "x", None),
            P(orb, "x", None),
        ),
        out_specs=P(orb, "x", None),
        check_vma=False,
    )
```

```python
import jax
import jax.numpy as jnp
import numpy as np
from jax import lax
from jax.experimental import pallas as pl
from jax.experimental.pallas import tpu as pltpu
from jax.sharding import Mesh, PartitionSpec as P

FIELDS = 4
PAD = 8
UNROLL = 4
OWNER_BIT = 20
ENTRY_BITS = 7


def tile_kernel(side):
    blocks = side // 8
    pitch = side + PAD
    reach = FIELDS * pitch

    def kernel(core_ref, count_ref, code_ref, own_ref, peer_ref, out_ref, pairs):
        lane = lax.broadcasted_iota(jnp.int32, (8, 128), 1)
        row = lax.broadcasted_iota(jnp.int32, (8, 128), 0)
        zero = jnp.zeros((8, 128), jnp.float32)
        keep_z = (lane % 32) < 31

        def boxes(ref, index, a):
            here = [
                ref[(*index, pl.ds(a * side + 8 * j, 8))].astype(jnp.float32)
                for j in range(blocks)
            ]
            edge = ref[(*index, pl.ds(2 * side + 8 * a, 8))].astype(jnp.float32)
            turned = [pltpu.roll(v, 7, 0) for v in here] + [zero]
            up_x = [jnp.where(row < 7, turned[j], turned[j + 1]) for j in range(blocks)]
            up_y = []
            for j in range(blocks):
                shift = (96 - 32 * j) % 128
                beyond = pltpu.roll(edge, shift, 1) if shift else edge
                up_y.append(jnp.where(lane < 96, pltpu.roll(here[j], 96, 1), beyond))
            up_z = [pltpu.roll(v, 127, 1) for v in here]
            return here, up_x, up_y, up_z

        def build(peer, _):
            for a in range(2):
                here, up_x, up_y, up_z = boxes(peer_ref, (peer,), a)
                base = pl.multiple_of((peer * 2 + a) * reach, 8)
                for k, other in enumerate((here, up_x, up_y, up_z)):
                    pairs[pl.ds(base + k * pitch, 8)] = zero
                    for j in range(blocks):
                        pairs[pl.ds(base + k * pitch + PAD + 8 * j, 8)] = here[j] * other[j]
            return 0

        peers = peer_ref.shape[0]
        lax.fori_loop(0, peers, build, 0)
        pairs[pl.ds(peers * 2 * reach, PAD)] = zero

        def finish(own, _):
            edges = []
            for a in range(2):
                first = count_ref[own, 0] if a else jnp.int32(0)
                count = count_ref[own, a]

                def add(index, sums):
                    start = (code_ref[own, index] & ((1 << OWNER_BIT) - 1)) >> ENTRY_BITS
                    return [
                        sums[k * blocks + j] + pairs[pl.ds(start + k * pitch + 8 * j, 8)]
                        for k in range(FIELDS)
                        for j in range(blocks)
                    ]

                def several(g, sums):
                    for u in range(UNROLL):
                        sums = add(first + g * UNROLL + u, sums)
                    return sums

                groups = count // UNROLL
                sums = [zero] * (FIELDS * blocks)
                sums = lax.fori_loop(0, groups, several, sums)
                sums = lax.fori_loop(
                    first + groups * UNROLL, first + count, lambda i, s: add(i, s), sums
                )
                here, up_x, up_y, up_z = boxes(own_ref, (own, core_ref[0]), a)
                before = zero
                for j in range(blocks):
                    self_sum, along_x, along_y, along_z = [
                        sums[k * blocks + j] for k in range(FIELDS)
                    ]
                    along_z = jnp.where(keep_z, along_z, 0.0)
                    back_x = pltpu.roll(here[j] * along_x, 1, 0)
                    back_y = here[j] * along_y
                    back_z = pltpu.roll(here[j] * along_z, 1, 1)
                    total = up_x[j] * along_x + jnp.where(row > 0, back_x, before)
                    total = total + up_y[j] * along_y
                    total = total + jnp.where(lane >= 32, pltpu.roll(back_y, 32, 1), 0.0)
                    total = total + (up_z[j] * along_z + back_z)
                    before = back_x
                    total = (here[j] * self_sum + total / 6.0) / 6.0
                    chunk = own * blocks + j
                    out_ref[chunk, pl.ds(8 * a, 8)] = total.astype(out_ref.dtype)
                    past = pltpu.roll(back_y, 32 + 32 * a, 1) / 36.0
                    if a == 0:
                        edges.append(past)
                    else:
                        both = jnp.where(lane < 32, edges[j], past)
                        out_ref[chunk, pl.ds(16, 8)] = both.astype(out_ref.dtype)
            return 0

        lax.fori_loop(0, own_ref.shape[0], finish, 0)

    return kernel


def apply_tile(core, counts, codes, own, peer, side, interpret=False):
    blocks = side // 8
    rows = peer.shape[0] * 2 * FIELDS * (side + PAD) + PAD
    smem = pl.BlockSpec(memory_space=pltpu.SMEM)
    vmem = pl.BlockSpec(memory_space=pltpu.VMEM)
    return pl.pallas_call(
        tile_kernel(side),
        out_shape=jax.ShapeDtypeStruct((own.shape[0] * blocks, 24, 128), jnp.bfloat16),
        in_specs=[smem, smem, smem, vmem, vmem],
        out_specs=vmem,
        scratch_shapes=[pltpu.VMEM((rows, 128), jnp.float32)],
        compiler_params=pltpu.CompilerParams(vmem_limit_bytes=16 * 1024 * 1024),
        interpret=interpret,
    )(core, counts, codes, own, peer)


def tasks_of(own_meta, peer_meta, side):
    reach = FIELDS * (side + PAD)
    peers = own_meta.shape[2]
    base = jnp.arange(peers, dtype=jnp.int32)[None, :, None] * 2

    def keys(owner, partner, back):
        start = (base + partner) * reach + PAD - back
        return jnp.where(owner >= 0, (owner << OWNER_BIT) + (start << ENTRY_BITS), 4 << OWNER_BIT)

    as_left = keys(own_meta[1], peer_meta[0], own_meta[2])
    as_right = keys(own_meta[0], peer_meta[1], -peer_meta[2])
    owners = jnp.concatenate([own_meta[1], own_meta[0]], 1).reshape(own_meta.shape[1], -1)
    codes = jnp.concatenate([as_left, as_right], 1).reshape(own_meta.shape[1], -1)
    codes = codes + jnp.arange(codes.shape[1], dtype=jnp.int32)
    counts = jnp.stack([jnp.sum(owners == a, 1, dtype=jnp.int32) for a in range(2)], 1)
    rank = jnp.sum(codes[:, None, :] < codes[:, :, None], 2, dtype=jnp.int32)
    slot = jnp.arange(codes.shape[1], dtype=jnp.int32)
    placed = jnp.where(rank[:, None, :] == slot[None, :, None], codes[:, None, :], 0)
    return counts, jnp.sum(placed, 2, dtype=jnp.int32)


def payload_of(rounded, meta, slab):
    owned, side, _ = rounded.shape
    wide = jnp.pad(rounded, ((0, 0), (0, 0), (0, 128)))
    part = lax.dynamic_slice(wide, (0, 0, slab * 128), (owned, side, 128 + side))
    edge = part[:, :, 128:].reshape(owned, side // 8, 8, side)
    edge = jnp.moveaxis(edge, 1, 2).reshape(owned * 8, 128)
    return jnp.concatenate([part[:, :, :128].reshape(owned * side, 128), edge, meta], 0)


def meta_of(received, kinds, pairs):
    meta = received[:, 80 : 80 + kinds * pairs].astype(jnp.int32)
    return meta.reshape(received.shape[0], pairs, kinds, 128)


def local(orbitals, send_index, pair_left, pair_offset):
    owned, side, width = orbitals.shape
    pairs = lax.axis_size("x")
    cores = lax.axis_size("c")
    z_size = lax.axis_size("z")
    y_size = lax.axis_size("y")
    x = lax.axis_index("x")
    y = lax.axis_index("y")
    z = lax.axis_index("z")
    rounded = orbitals.astype(jnp.bfloat16)
    meta = jnp.stack([send_index.reshape(-1), pair_left.reshape(-1), pair_offset.reshape(-1)])
    meta = jnp.broadcast_to(meta.astype(jnp.bfloat16)[None], (pairs, 3, 128))
    meta = lax.all_to_all(meta, "x", 0, 0, tiled=True).reshape(pairs * 3, 128)
    meta = jnp.pad(meta, ((0, 4), (0, 0)))
    payload = jnp.stack([payload_of(rounded, meta, c * pairs + x) for c in range(cores)])
    to_peers = jnp.broadcast_to(payload[None], (y_size,) + payload.shape)
    to_peers = to_peers.reshape((y_size * cores,) + payload.shape[1:])
    peer = lax.all_to_all(to_peers, ("y", "c"), 0, 0, tiled=True)
    own = lax.all_gather(payload, ("z", "c"), axis=0, tiled=False)

    own_meta = meta_of(own[:, 0], 3, pairs)
    own_meta = lax.dynamic_slice_in_dim(own_meta, z * (y_size * cores), y_size * cores, 3)
    own_meta = jnp.transpose(own_meta, (2, 0, 3, 1))
    peer_meta = meta_of(peer, 3, pairs).reshape(-1, pairs, 3, z_size, y_size, cores)
    peer_meta = lax.dynamic_index_in_dim(peer_meta, y, 4, keepdims=False)
    peer_meta = peer_meta.reshape(-1, pairs, 3, z_size * cores)
    peer_meta = jnp.transpose(peer_meta, (2, 3, 0, 1))
    counts, codes = tasks_of(own_meta, peer_meta, side)

    core = lax.axis_index("c").astype(jnp.int32).reshape(1)
    partial = apply_tile(core, counts, codes, own, peer, side)
    landed = lax.all_to_all(partial, ("z", "c", "x"), 0, 0, tiled=True)
    landed = landed.reshape(z_size, cores * pairs, 24, 128).astype(jnp.float32)
    slabs = jnp.sum(landed, 0)
    field = slabs[:, :16].reshape(cores * pairs, owned, 8, 128)
    edge = slabs[:-1, 16:, : owned * 32].reshape(-1, 8, owned, 32)
    edge = jnp.moveaxis(edge, 2, 1)
    field = field + jnp.pad(edge, ((1, 0), (0, 0), (0, 0), (0, 96)))
    field = -0.25 * field
    return jnp.transpose(field, (1, 2, 0, 3)).reshape(owned, 8, width)


def solution(mesh):
    fine = Mesh(np.asarray(mesh.devices).reshape(8, 8, 2, 4), ("z", "y", "c", "x"))
    orb = ("z", "y", "c")
    return jax.shard_map(
        local,
        mesh=fine,
        in_specs=(
            P(orb, None, None),
            P(orb, "x", None),
            P(orb, "x", None),
            P(orb, "x", None),
        ),
        out_specs=P(orb, "x", None),
        check_vma=False,
    )
```

```python
import jax
import jax.numpy as jnp
import numpy as np
from jax import lax
from jax.experimental import pallas as pl
from jax.experimental.pallas import tpu as pltpu
from jax.sharding import Mesh, PartitionSpec as P

FIELDS = 4
PAD = 8
UNROLL = 8
BUILD_STEP = 4
FINISH_STEP = 4
OWNER_BIT = 20
ENTRY_BITS = 7


def tile_kernel(side):
    blocks = side // 8
    pitch = side + PAD
    reach = FIELDS * pitch

    def kernel(core_ref, count_ref, code_ref, own_ref, peer_ref, out_ref, pairs, totals):
        lane = lax.broadcasted_iota(jnp.int32, (8, 128), 1)
        row = lax.broadcasted_iota(jnp.int32, (8, 128), 0)
        zero = jnp.zeros((8, 128), jnp.float32)
        keep_z = (lane % 32) < 31

        def boxes(ref, index, a):
            here = [
                ref[(*index, pl.ds(a * side + 8 * j, 8))].astype(jnp.float32)
                for j in range(blocks)
            ]
            edge = ref[(*index, pl.ds(2 * side + 8 * a, 8))].astype(jnp.float32)
            turned = [pltpu.roll(v, 7, 0) for v in here] + [zero]
            up_x = [jnp.where(row < 7, turned[j], turned[j + 1]) for j in range(blocks)]
            up_y = []
            for j in range(blocks):
                shift = (96 - 32 * j) % 128
                beyond = pltpu.roll(edge, shift, 1) if shift else edge
                up_y.append(jnp.where(lane < 96, pltpu.roll(here[j], 96, 1), beyond))
            up_z = [pltpu.roll(v, 127, 1) for v in here]
            return here, up_x, up_y, up_z

        def build(step, _):
            for u in range(BUILD_STEP):
                peer = step * BUILD_STEP + u
                for a in range(2):
                    here, up_x, up_y, up_z = boxes(peer_ref, (peer,), a)
                    base = pl.multiple_of((peer * 2 + a) * reach, 8)
                    for k, other in enumerate((here, up_x, up_y, up_z)):
                        pairs[pl.ds(base + k * pitch, 8)] = zero
                        for j in range(blocks):
                            pairs[pl.ds(base + k * pitch + PAD + 8 * j, 8)] = here[j] * other[j]
            return 0

        peers = peer_ref.shape[0]
        owners = own_ref.shape[0]
        entries = code_ref.shape[1]
        nothing = peers * 2 * reach
        lax.fori_loop(0, peers // BUILD_STEP, build, 0)
        for i in range(reach // 8):
            pairs[pl.ds(nothing + 8 * i, 8)] = zero

        def gather(own, _):
            for a in range(2):
                first = count_ref[own, 0] if a else jnp.int32(0)
                last = first + count_ref[own, a]

                def several(g, sums):
                    for u in range(UNROLL):
                        index = first + g * UNROLL + u
                        code = code_ref[own, jnp.minimum(index, entries - 1)]
                        start = (code & ((1 << OWNER_BIT) - 1)) >> ENTRY_BITS
                        start = jnp.where(index < last, start, nothing)
                        sums = [
                            sums[k * blocks + j] + pairs[pl.ds(start + k * pitch + 8 * j, 8)]
                            for k in range(FIELDS)
                            for j in range(blocks)
                        ]
                    return sums

                groups = (last - first + UNROLL - 1) // UNROLL
                sums = lax.fori_loop(0, groups, several, [zero] * (FIELDS * blocks))
                for i, value in enumerate(sums):
                    totals[own, a, i] = value
            return 0

        lax.fori_loop(0, owners, gather, 0)

        def finish(step, _):
            for u in range(FINISH_STEP):
                own = step * FINISH_STEP + u
                edges = []
                for a in range(2):
                    here, up_x, up_y, up_z = boxes(own_ref, (own, core_ref[0]), a)
                    before = zero
                    for j in range(blocks):
                        self_sum, along_x, along_y, along_z = [
                            totals[own, a, k * blocks + j] for k in range(FIELDS)
                        ]
                        along_z = jnp.where(keep_z, along_z, 0.0)
                        back_x = pltpu.roll(here[j] * along_x, 1, 0)
                        back_y = pltpu.roll(here[j] * along_y, 32, 1)
                        back_z = pltpu.roll(here[j] * along_z, 1, 1)
                        total = up_x[j] * along_x + jnp.where(row > 0, back_x, before)
                        total = total + up_y[j] * along_y + jnp.where(lane >= 32, back_y, 0.0)
                        total = total + (up_z[j] * along_z + back_z)
                        before = back_x
                        total = (here[j] * self_sum + total / 6.0) / 6.0
                        chunk = own * blocks + j
                        out_ref[chunk, pl.ds(8 * a, 8)] = total.astype(out_ref.dtype)
                        if a == 0:
                            edges.append(back_y)
                        else:
                            both = jnp.where(lane < 32, edges[j], pltpu.roll(back_y, 32, 1))
                            out_ref[chunk, pl.ds(16, 8)] = (both / 36.0).astype(out_ref.dtype)
            return 0

        lax.fori_loop(0, owners // FINISH_STEP, finish, 0)

    return kernel


def apply_tile(core, counts, codes, own, peer, side, interpret=False):
    blocks = side // 8
    rows = (peer.shape[0] * 2 + 1) * FIELDS * (side + PAD)
    smem = pl.BlockSpec(memory_space=pltpu.SMEM)
    vmem = pl.BlockSpec(memory_space=pltpu.VMEM)
    return pl.pallas_call(
        tile_kernel(side),
        out_shape=jax.ShapeDtypeStruct((own.shape[0] * blocks, 24, 128), jnp.bfloat16),
        in_specs=[smem, smem, smem, vmem, vmem],
        out_specs=vmem,
        scratch_shapes=[
            pltpu.VMEM((rows, 128), jnp.float32),
            pltpu.VMEM((own.shape[0], 2, FIELDS * blocks, 8, 128), jnp.float32),
        ],
        compiler_params=pltpu.CompilerParams(vmem_limit_bytes=16 * 1024 * 1024),
        interpret=interpret,
    )(core, counts, codes, own, peer)


def tasks_of(own_meta, peer_meta, side):
    reach = FIELDS * (side + PAD)
    peers = own_meta.shape[2]
    base = jnp.arange(peers, dtype=jnp.int32)[None, :, None] * 2

    def keys(owner, partner, back):
        start = (base + partner) * reach + PAD - back
        return jnp.where(owner >= 0, (owner << OWNER_BIT) + (start << ENTRY_BITS), 4 << OWNER_BIT)

    as_left = keys(own_meta[1], peer_meta[0], own_meta[2])
    as_right = keys(own_meta[0], peer_meta[1], -peer_meta[2])
    owners = jnp.concatenate([own_meta[1], own_meta[0]], 1).reshape(own_meta.shape[1], -1)
    codes = jnp.concatenate([as_left, as_right], 1).reshape(own_meta.shape[1], -1)
    codes = codes + jnp.arange(codes.shape[1], dtype=jnp.int32)
    counts = jnp.stack([jnp.sum(owners == a, 1, dtype=jnp.int32) for a in range(2)], 1)
    rank = jnp.sum(codes[:, None, :] < codes[:, :, None], 2, dtype=jnp.int32)
    slot = jnp.arange(codes.shape[1], dtype=jnp.int32)
    placed = jnp.where(rank[:, None, :] == slot[None, :, None], codes[:, None, :], 0)
    return counts, jnp.sum(placed, 2, dtype=jnp.int32)


def payload_of(rounded, meta, slab):
    owned, side, _ = rounded.shape
    wide = jnp.pad(rounded, ((0, 0), (0, 0), (0, 128)))
    part = lax.dynamic_slice(wide, (0, 0, slab * 128), (owned, side, 128 + side))
    edge = part[:, :, 128:].reshape(owned, side // 8, 8, side)
    edge = jnp.moveaxis(edge, 1, 2).reshape(owned * 8, 128)
    return jnp.concatenate([part[:, :, :128].reshape(owned * side, 128), edge, meta], 0)


def meta_of(received, kinds, pairs):
    meta = received[:, 80 : 80 + kinds * pairs].astype(jnp.int32)
    return meta.reshape(received.shape[0], pairs, kinds, 128)


def local(orbitals, send_index, pair_left, pair_offset):
    owned, side, width = orbitals.shape
    pairs = lax.axis_size("x")
    cores = lax.axis_size("c")
    z_size = lax.axis_size("z")
    y_size = lax.axis_size("y")
    x = lax.axis_index("x")
    y = lax.axis_index("y")
    z = lax.axis_index("z")
    rounded = orbitals.astype(jnp.bfloat16)
    meta = jnp.stack([send_index.reshape(-1), pair_left.reshape(-1), pair_offset.reshape(-1)])
    meta = jnp.broadcast_to(meta.astype(jnp.bfloat16)[None], (pairs, 3, 128))
    meta = lax.all_to_all(meta, "x", 0, 0, tiled=True).reshape(pairs * 3, 128)
    meta = jnp.pad(meta, ((0, 4), (0, 0)))
    payload = jnp.stack([payload_of(rounded, meta, c * pairs + x) for c in range(cores)])
    to_peers = jnp.broadcast_to(payload[None], (y_size,) + payload.shape)
    to_peers = to_peers.reshape((y_size * cores,) + payload.shape[1:])
    peer = lax.all_to_all(to_peers, ("y", "c"), 0, 0, tiled=True)
    own = lax.all_gather(payload, ("z", "c"), axis=0, tiled=False)

    own_meta = meta_of(own[:, 0], 3, pairs)
    own_meta = lax.dynamic_slice_in_dim(own_meta, z * (y_size * cores), y_size * cores, 3)
    own_meta = jnp.transpose(own_meta, (2, 0, 3, 1))
    peer_meta = meta_of(peer, 3, pairs).reshape(-1, pairs, 3, z_size, y_size, cores)
    peer_meta = lax.dynamic_index_in_dim(peer_meta, y, 4, keepdims=False)
    peer_meta = peer_meta.reshape(-1, pairs, 3, z_size * cores)
    peer_meta = jnp.transpose(peer_meta, (2, 3, 0, 1))
    counts, codes = tasks_of(own_meta, peer_meta, side)

    core = lax.axis_index("c").astype(jnp.int32).reshape(1)
    partial = apply_tile(core, counts, codes, own, peer, side)
    landed = lax.all_to_all(partial, ("z", "c", "x"), 0, 0, tiled=True)
    landed = landed.reshape(z_size, cores * pairs, 24, 128).astype(jnp.float32)
    slabs = jnp.sum(landed, 0)
    field = slabs[:, :16].reshape(cores * pairs, owned, 8, 128)
    edge = slabs[:-1, 16:, : owned * 32].reshape(-1, 8, owned, 32)
    edge = jnp.moveaxis(edge, 2, 1)
    field = field + jnp.pad(edge, ((1, 0), (0, 0), (0, 0), (0, 96)))
    field = -0.25 * field
    return jnp.transpose(field, (1, 2, 0, 3)).reshape(owned, 8, width)


def solution(mesh):
    fine = Mesh(np.asarray(mesh.devices).reshape(8, 8, 2, 4), ("z", "y", "c", "x"))
    orb = ("z", "y", "c")
    return jax.shard_map(
        local,
        mesh=fine,
        in_specs=(
            P(orb, None, None),
            P(orb, "x", None),
            P(orb, "x", None),
            P(orb, "x", None),
        ),
        out_specs=P(orb, "x", None),
        check_vma=False,
    )
```

```python
import jax
import jax.numpy as jnp
import numpy as np
from jax import lax
from jax.experimental import pallas as pl
from jax.experimental.pallas import tpu as pltpu
from jax.sharding import Mesh, PartitionSpec as P

FIELDS = 4
PAD = 8
UNROLL = 5
BUILD_STEP = 8
FINISH_STEP = 4
OWNER_BIT = 20
ENTRY_BITS = 7


def tile_kernel(side):
    blocks = side // 8
    pitch = side + PAD
    reach = FIELDS * pitch

    def kernel(core_ref, count_ref, code_ref, own_ref, peer_ref, out_ref, pairs, totals):
        lane = lax.broadcasted_iota(jnp.int32, (8, 128), 1)
        row = lax.broadcasted_iota(jnp.int32, (8, 128), 0)
        zero = jnp.zeros((8, 128), jnp.float32)
        keep_z = (lane % 32) < 31

        def boxes(ref, index, a, first):
            here = [
                ref[index, pl.ds(first + a * side + 8 * j, 8)].astype(jnp.float32)
                for j in range(blocks)
            ]
            edge = ref[index, pl.ds(first + 2 * side + 8 * a, 8)].astype(jnp.float32)
            turned = [pltpu.roll(v, 7, 0) for v in here] + [zero]
            up_x = [jnp.where(row < 7, turned[j], turned[j + 1]) for j in range(blocks)]
            up_y = []
            for j in range(blocks):
                shift = (96 - 32 * j) % 128
                beyond = pltpu.roll(edge, shift, 1) if shift else edge
                up_y.append(jnp.where(lane < 96, pltpu.roll(here[j], 96, 1), beyond))
            up_z = [pltpu.roll(v, 127, 1) for v in here]
            return here, up_x, up_y, up_z

        def build(step, _):
            for u in range(BUILD_STEP):
                peer = step * BUILD_STEP + u
                for a in range(2):
                    here, up_x, up_y, up_z = boxes(peer_ref, peer, a, 0)
                    base = pl.multiple_of((peer * 2 + a) * reach, 8)
                    for k, other in enumerate((here, up_x, up_y, up_z)):
                        pairs[pl.ds(base + k * pitch, 8)] = zero
                        for j in range(blocks):
                            pairs[pl.ds(base + k * pitch + PAD + 8 * j, 8)] = here[j] * other[j]
            return 0

        peers = peer_ref.shape[0]
        owners = own_ref.shape[0]
        entries = code_ref.shape[1]
        nothing = peers * 2 * reach
        lax.fori_loop(0, peers // BUILD_STEP, build, 0)
        for i in range(reach // 8):
            pairs[pl.ds(nothing + 8 * i, 8)] = zero

        def gather(own, _):
            for a in range(2):
                first = count_ref[own, 0] if a else jnp.int32(0)
                last = first + count_ref[own, a]

                def starts_of(g):
                    starts = []
                    for u in range(UNROLL):
                        index = first + g * UNROLL + u
                        code = code_ref[own, jnp.minimum(index, entries - 1)]
                        start = (code & ((1 << OWNER_BIT) - 1)) >> ENTRY_BITS
                        starts.append(jnp.where(index < last, start, nothing))
                    return starts

                def several(g, carried):
                    sums, starts = carried
                    following = starts_of(g + 1)
                    for start in starts:
                        sums = [
                            sums[k * blocks + j] + pairs[pl.ds(start + k * pitch + 8 * j, 8)]
                            for k in range(FIELDS)
                            for j in range(blocks)
                        ]
                    return sums, following

                groups = (last - first + UNROLL - 1) // UNROLL
                none = [zero] * (FIELDS * blocks)
                sums, _ = lax.fori_loop(0, groups, several, (none, starts_of(0)))
                for i, value in enumerate(sums):
                    totals[own, a, i] = value
            return 0

        lax.fori_loop(0, owners, gather, 0)

        slab = pl.multiple_of(core_ref[0] * (2 * side + 16), 16)

        def finish(step, _):
            for u in range(FINISH_STEP):
                own = step * FINISH_STEP + u
                edges = []
                for a in range(2):
                    here, up_x, up_y, up_z = boxes(own_ref, own, a, slab)
                    before = zero
                    for j in range(blocks):
                        self_sum, along_x, along_y, along_z = [
                            totals[own, a, k * blocks + j] for k in range(FIELDS)
                        ]
                        along_z = jnp.where(keep_z, along_z, 0.0)
                        back_x = pltpu.roll(here[j] * along_x, 1, 0)
                        back_y = pltpu.roll(here[j] * along_y, 32, 1)
                        back_z = pltpu.roll(here[j] * along_z, 1, 1)
                        total = up_x[j] * along_x + jnp.where(row > 0, back_x, before)
                        total = total + up_y[j] * along_y + jnp.where(lane >= 32, back_y, 0.0)
                        total = total + (up_z[j] * along_z + back_z)
                        before = back_x
                        total = (here[j] * self_sum + total / 6.0) / 6.0
                        chunk = own * blocks + j
                        out_ref[chunk, pl.ds(8 * a, 8)] = total.astype(out_ref.dtype)
                        if a == 0:
                            edges.append(back_y)
                        else:
                            both = jnp.where(lane < 32, edges[j], pltpu.roll(back_y, 32, 1))
                            out_ref[chunk, pl.ds(16, 8)] = (both / 36.0).astype(out_ref.dtype)
            return 0

        lax.fori_loop(0, owners // FINISH_STEP, finish, 0)

    return kernel


def apply_tile(core, counts, codes, own, peer, side, interpret=False):
    blocks = side // 8
    rows = (peer.shape[0] * 2 + 1) * FIELDS * (side + PAD)
    smem = pl.BlockSpec(memory_space=pltpu.SMEM)
    vmem = pl.BlockSpec(memory_space=pltpu.VMEM)
    return pl.pallas_call(
        tile_kernel(side),
        out_shape=jax.ShapeDtypeStruct((own.shape[0] * blocks, 24, 128), jnp.bfloat16),
        in_specs=[smem, smem, smem, vmem, vmem],
        out_specs=vmem,
        scratch_shapes=[
            pltpu.VMEM((rows, 128), jnp.float32),
            pltpu.VMEM((own.shape[0], 2, FIELDS * blocks, 8, 128), jnp.float32),
        ],
        compiler_params=pltpu.CompilerParams(vmem_limit_bytes=16 * 1024 * 1024),
        interpret=interpret,
    )(core, counts, codes, own, peer)


def tasks_of(own_meta, peer_meta, side):
    reach = FIELDS * (side + PAD)
    peers = own_meta.shape[2]
    base = jnp.arange(peers, dtype=jnp.int32)[None, :, None] * 2

    def keys(owner, partner, back):
        start = (base + partner) * reach + PAD - back
        return jnp.where(owner >= 0, (owner << OWNER_BIT) + (start << ENTRY_BITS), 4 << OWNER_BIT)

    as_left = keys(own_meta[1], peer_meta[0], own_meta[2])
    as_right = keys(own_meta[0], peer_meta[1], -peer_meta[2])
    owners = jnp.concatenate([own_meta[1], own_meta[0]], 1).reshape(own_meta.shape[1], -1)
    codes = jnp.concatenate([as_left, as_right], 1).reshape(own_meta.shape[1], -1)
    codes = codes + jnp.arange(codes.shape[1], dtype=jnp.int32)
    counts = jnp.stack([jnp.sum(owners == a, 1, dtype=jnp.int32) for a in range(2)], 1)
    rank = jnp.sum(codes[:, None, :] < codes[:, :, None], 2, dtype=jnp.int32)
    slot = jnp.arange(codes.shape[1], dtype=jnp.int32)
    placed = jnp.where(rank[:, None, :] == slot[None, :, None], codes[:, None, :], 0)
    return counts, jnp.sum(placed, 2, dtype=jnp.int32)


def payloads_of(rounded, meta, x):
    owned, side, _ = rounded.shape
    wide = jnp.pad(rounded, ((0, 0), (0, 0), (0, 128)))
    part = lax.dynamic_slice(wide, (0, 0, x * 256), (owned, side, 256 + side))

    def folded(edge):
        edge = edge.reshape(owned, side // 8, 8, side)
        return jnp.moveaxis(edge, 1, 2).reshape(owned * 8, 128)

    mains = [part[:, :, c * 128 : c * 128 + 128].reshape(owned * side, 128) for c in range(2)]
    edges = [folded(part[:, :, c * 128 + 128 : c * 128 + 128 + side]) for c in range(2)]
    peer = jnp.stack([jnp.concatenate([mains[c], edges[c], meta], 0) for c in range(2)])
    own = jnp.concatenate([mains[0], edges[0], mains[1], edges[1], meta], 0)
    return peer, own


def meta_of(received, kinds, pairs):
    first = received.shape[1] - 16
    meta = received[:, first : first + kinds * pairs].astype(jnp.int32)
    return meta.reshape(received.shape[0], pairs, kinds, 128)


def local(orbitals, send_index, pair_left, pair_offset):
    owned, side, width = orbitals.shape
    pairs = lax.axis_size("x")
    cores = lax.axis_size("c")
    z_size = lax.axis_size("z")
    y_size = lax.axis_size("y")
    x = lax.axis_index("x")
    y = lax.axis_index("y")
    z = lax.axis_index("z")
    rounded = orbitals.astype(jnp.bfloat16)
    meta = jnp.stack([send_index.reshape(-1), pair_left.reshape(-1), pair_offset.reshape(-1)])
    meta = jnp.broadcast_to(meta.astype(jnp.bfloat16)[None], (pairs, 3, 128))
    meta = lax.all_to_all(meta, "x", 0, 0, tiled=True).reshape(pairs * 3, 128)
    meta = jnp.pad(meta, ((0, 4), (0, 0)))
    payload, own_payload = payloads_of(rounded, meta, x)
    to_peers = jnp.broadcast_to(payload[None], (y_size,) + payload.shape)
    to_peers = to_peers.reshape((y_size * cores,) + payload.shape[1:])
    peer = lax.all_to_all(to_peers, ("y", "c"), 0, 0, tiled=True)
    own = lax.all_gather(own_payload, ("z", "c"), axis=0, tiled=False)

    own_meta = meta_of(own, 3, pairs)
    own_meta = lax.dynamic_slice_in_dim(own_meta, z * (y_size * cores), y_size * cores, 3)
    own_meta = jnp.transpose(own_meta, (2, 0, 3, 1))
    peer_meta = meta_of(peer, 3, pairs).reshape(-1, pairs, 3, z_size, y_size, cores)
    peer_meta = lax.dynamic_index_in_dim(peer_meta, y, 4, keepdims=False)
    peer_meta = peer_meta.reshape(-1, pairs, 3, z_size * cores)
    peer_meta = jnp.transpose(peer_meta, (2, 3, 0, 1))
    counts, codes = tasks_of(own_meta, peer_meta, side)

    core = lax.axis_index("c").astype(jnp.int32).reshape(1)
    partial = apply_tile(core, counts, codes, own, peer, side)
    landed = lax.all_to_all(partial, ("z", "c", "x"), 0, 0, tiled=True)
    landed = landed.reshape(z_size, cores, pairs, 24, 128).astype(jnp.float32)
    slabs = jnp.moveaxis(jnp.sum(landed, 0), 0, 1).reshape(cores * pairs, 24, 128)
    field = slabs[:, :16].reshape(cores * pairs, owned, 8, 128)
    edge = slabs[:-1, 16:, : owned * 32].reshape(-1, 8, owned, 32)
    edge = jnp.moveaxis(edge, 2, 1)
    field = field + jnp.pad(edge, ((1, 0), (0, 0), (0, 0), (0, 96)))
    field = -0.25 * field
    return jnp.transpose(field, (1, 2, 0, 3)).reshape(owned, 8, width)


def solution(mesh):
    fine = Mesh(np.asarray(mesh.devices).reshape(8, 8, 2, 4), ("z", "y", "c", "x"))
    orb = ("z", "y", "c")
    return jax.shard_map(
        local,
        mesh=fine,
        in_specs=(
            P(orb, None, None),
            P(orb, "x", None),
            P(orb, "x", None),
            P(orb, "x", None),
        ),
        out_specs=P(orb, "x", None),
        check_vma=False,
    )
```

```python
import jax
import jax.numpy as jnp
import numpy as np
from jax import lax
from jax.experimental import pallas as pl
from jax.experimental.pallas import tpu as pltpu
from jax.sharding import Mesh, PartitionSpec as P

FIELDS = 4
PAD = 8
UNROLL = 4
BUILD_STEP = 4
FINISH_STEP = 4
OWNER_BIT = 20
ENTRY_BITS = 7


def tile_kernel(side):
    blocks = side // 8
    pitch = side + PAD
    reach = FIELDS * pitch

    def kernel(core_ref, count_ref, code_ref, own_ref, peer_ref, out_ref, pairs, totals):
        lane = lax.broadcasted_iota(jnp.int32, (8, 128), 1)
        row = lax.broadcasted_iota(jnp.int32, (8, 128), 0)
        zero = jnp.zeros((8, 128), jnp.float32)
        keep_z = (lane % 32) < 31

        def boxes(ref, index, a, first):
            here = [
                ref[index, pl.ds(first + a * side + 8 * j, 8)].astype(jnp.float32)
                for j in range(blocks)
            ]
            edge = ref[index, pl.ds(first + 2 * side + 8 * a, 8)].astype(jnp.float32)
            turned = [pltpu.roll(v, 7, 0) for v in here] + [zero]
            up_x = [jnp.where(row < 7, turned[j], turned[j + 1]) for j in range(blocks)]
            up_y = []
            for j in range(blocks):
                shift = (96 - 32 * j) % 128
                beyond = pltpu.roll(edge, shift, 1) if shift else edge
                up_y.append(jnp.where(lane < 96, pltpu.roll(here[j], 96, 1), beyond))
            up_z = [pltpu.roll(v, 127, 1) for v in here]
            return here, up_x, up_y, up_z

        def build(step, _):
            for u in range(BUILD_STEP):
                peer = step * BUILD_STEP + u
                for a in range(2):
                    here, up_x, up_y, up_z = boxes(peer_ref, peer, a, 0)
                    base = pl.multiple_of((peer * 2 + a) * reach, 8)
                    for k, other in enumerate((here, up_x, up_y, up_z)):
                        pairs[pl.ds(base + k * pitch, 8)] = zero
                        for j in range(blocks):
                            pairs[pl.ds(base + k * pitch + PAD + 8 * j, 8)] = here[j] * other[j]
            return 0

        peers = peer_ref.shape[0]
        owners = own_ref.shape[0]
        entries = code_ref.shape[1]
        nothing = peers * 2 * reach
        lax.fori_loop(0, peers // BUILD_STEP, build, 0)
        for i in range(reach // 8):
            pairs[pl.ds(nothing + 8 * i, 8)] = zero

        def gather(own, _):
            for a in range(2):
                first = count_ref[own, 0] if a else jnp.int32(0)
                last = first + count_ref[own, a]

                def starts_of(g):
                    starts = []
                    for u in range(UNROLL):
                        index = first + g * UNROLL + u
                        code = code_ref[own, jnp.minimum(index, entries - 1)]
                        start = (code & ((1 << OWNER_BIT) - 1)) >> ENTRY_BITS
                        starts.append(jnp.where(index < last, start, nothing))
                    return starts

                def several(g, carried):
                    sums, starts = carried
                    following = starts_of(g + 1)
                    for start in starts:
                        sums = [
                            sums[k * blocks + j] + pairs[pl.ds(start + k * pitch + 8 * j, 8)]
                            for k in range(FIELDS)
                            for j in range(blocks)
                        ]
                    return sums, following

                groups = (last - first + UNROLL - 1) // UNROLL
                none = [zero] * (FIELDS * blocks)
                sums, _ = lax.fori_loop(0, groups, several, (none, starts_of(0)))
                for i, value in enumerate(sums):
                    totals[own, a, i] = value
            return 0

        lax.fori_loop(0, owners, gather, 0)

        slab = pl.multiple_of(core_ref[0] * (2 * side + 16), 16)

        def finish(step, _):
            for u in range(FINISH_STEP):
                own = step * FINISH_STEP + u
                edges = []
                for a in range(2):
                    here, up_x, up_y, up_z = boxes(own_ref, own, a, slab)
                    before = zero
                    for j in range(blocks):
                        self_sum, along_x, along_y, along_z = [
                            totals[own, a, k * blocks + j] for k in range(FIELDS)
                        ]
                        along_z = jnp.where(keep_z, along_z, 0.0)
                        back_x = pltpu.roll(here[j] * along_x, 1, 0)
                        back_y = pltpu.roll(here[j] * along_y, 32, 1)
                        back_z = pltpu.roll(here[j] * along_z, 1, 1)
                        total = up_x[j] * along_x + jnp.where(row > 0, back_x, before)
                        total = total + up_y[j] * along_y + jnp.where(lane >= 32, back_y, 0.0)
                        total = total + (up_z[j] * along_z + back_z)
                        before = back_x
                        total = (here[j] * self_sum + total / 6.0) / 6.0
                        chunk = own * blocks + j
                        out_ref[chunk, pl.ds(8 * a, 8)] = total.astype(out_ref.dtype)
                        if a == 0:
                            edges.append(back_y)
                        else:
                            both = jnp.where(lane < 32, edges[j], pltpu.roll(back_y, 32, 1))
                            out_ref[chunk, pl.ds(16, 8)] = (both / 36.0).astype(out_ref.dtype)
            return 0

        lax.fori_loop(0, owners // FINISH_STEP, finish, 0)

    return kernel


def apply_tile(core, counts, codes, own, peer, side, interpret=False):
    blocks = side // 8
    rows = (peer.shape[0] * 2 + 1) * FIELDS * (side + PAD)
    smem = pl.BlockSpec(memory_space=pltpu.SMEM)
    vmem = pl.BlockSpec(memory_space=pltpu.VMEM)
    return pl.pallas_call(
        tile_kernel(side),
        out_shape=jax.ShapeDtypeStruct((own.shape[0] * blocks, 24, 128), jnp.bfloat16),
        in_specs=[smem, smem, smem, vmem, vmem],
        out_specs=vmem,
        scratch_shapes=[
            pltpu.VMEM((rows, 128), jnp.float32),
            pltpu.VMEM((own.shape[0], 2, FIELDS * blocks, 8, 128), jnp.float32),
        ],
        compiler_params=pltpu.CompilerParams(vmem_limit_bytes=16 * 1024 * 1024),
        interpret=interpret,
    )(core, counts, codes, own, peer)


def tasks_of(own_meta, peer_meta, side):
    reach = FIELDS * (side + PAD)
    peers = own_meta.shape[2]
    base = jnp.arange(peers, dtype=jnp.int32)[None, :, None] * 2

    def keys(owner, partner, back):
        start = (base + partner) * reach + PAD - back
        return jnp.where(owner >= 0, (owner << OWNER_BIT) + (start << ENTRY_BITS), 4 << OWNER_BIT)

    as_left = keys(own_meta[1], peer_meta[0], own_meta[2])
    as_right = keys(own_meta[0], peer_meta[1], -peer_meta[2])
    owners = jnp.concatenate([own_meta[1], own_meta[0]], 1).reshape(own_meta.shape[1], -1)
    codes = jnp.concatenate([as_left, as_right], 1).reshape(own_meta.shape[1], -1)
    codes = codes + jnp.arange(codes.shape[1], dtype=jnp.int32)
    counts = jnp.stack([jnp.sum(owners == a, 1, dtype=jnp.int32) for a in range(2)], 1)
    rank = jnp.sum(codes[:, None, :] < codes[:, :, None], 2, dtype=jnp.int32)
    slot = jnp.arange(codes.shape[1], dtype=jnp.int32)
    placed = jnp.where(rank[:, None, :] == slot[None, :, None], codes[:, None, :], 0)
    return counts, jnp.sum(placed, 2, dtype=jnp.int32)


def payloads_of(rounded, meta, x):
    owned, side, _ = rounded.shape
    wide = jnp.pad(rounded, ((0, 0), (0, 0), (0, 128)))
    part = lax.dynamic_slice(wide, (0, 0, x * 256), (owned, side, 256 + side))

    def folded(edge):
        edge = edge.reshape(owned, side // 8, 8, side)
        return jnp.moveaxis(edge, 1, 2).reshape(owned * 8, 128)

    mains = [part[:, :, c * 128 : c * 128 + 128].reshape(owned * side, 128) for c in range(2)]
    edges = [folded(part[:, :, c * 128 + 128 : c * 128 + 128 + side]) for c in range(2)]
    peer = jnp.stack([jnp.concatenate([mains[c], edges[c], meta], 0) for c in range(2)])
    own = jnp.concatenate([mains[0], edges[0], mains[1], edges[1], meta], 0)
    return peer, own


def meta_of(received, kinds, pairs):
    first = received.shape[1] - 16
    meta = received[:, first : first + kinds * pairs].astype(jnp.int32)
    return meta.reshape(received.shape[0], pairs, kinds, 128)


def local(orbitals, send_index, pair_left, pair_offset):
    owned, side, width = orbitals.shape
    pairs = lax.axis_size("x")
    cores = lax.axis_size("c")
    z_size = lax.axis_size("z")
    y_size = lax.axis_size("y")
    x = lax.axis_index("x")
    y = lax.axis_index("y")
    z = lax.axis_index("z")
    rounded = orbitals.astype(jnp.bfloat16)
    meta = jnp.stack([send_index.reshape(-1), pair_left.reshape(-1), pair_offset.reshape(-1)])
    meta = jnp.broadcast_to(meta[None], (pairs, 3, 128))
    meta = lax.all_to_all(meta, "x", 0, 0, tiled=True).reshape(pairs * 3, 128)
    meta = jnp.pad(meta.astype(jnp.bfloat16), ((0, 4), (0, 0)))
    payload, own_payload = payloads_of(rounded, meta, x)
    to_peers = jnp.broadcast_to(payload[None], (y_size,) + payload.shape)
    to_peers = to_peers.reshape((y_size * cores,) + payload.shape[1:])
    peer = lax.all_to_all(to_peers, ("y", "c"), 0, 0, tiled=True)
    own = lax.all_gather(own_payload, ("z", "c"), axis=0, tiled=False)

    own_meta = meta_of(own, 3, pairs)
    own_meta = lax.dynamic_slice_in_dim(own_meta, z * (y_size * cores), y_size * cores, 3)
    own_meta = jnp.transpose(own_meta, (2, 0, 3, 1))
    peer_meta = meta_of(peer, 3, pairs).reshape(-1, pairs, 3, z_size, y_size, cores)
    peer_meta = lax.dynamic_index_in_dim(peer_meta, y, 4, keepdims=False)
    peer_meta = peer_meta.reshape(-1, pairs, 3, z_size * cores)
    peer_meta = jnp.transpose(peer_meta, (2, 3, 0, 1))
    counts, codes = tasks_of(own_meta, peer_meta, side)

    core = lax.axis_index("c").astype(jnp.int32).reshape(1)
    partial = apply_tile(core, counts, codes, own, peer, side)
    landed = lax.all_to_all(partial, ("z", "c", "x"), 0, 0, tiled=True)
    landed = landed.reshape(z_size, cores, pairs, 24, 128).astype(jnp.float32)
    slabs = jnp.moveaxis(jnp.sum(landed, 0), 0, 1).reshape(cores * pairs, 24, 128)
    field = slabs[:, :16].reshape(cores * pairs, owned, 8, 128)
    edge = slabs[:-1, 16:, : owned * 32].reshape(-1, 8, owned, 32)
    edge = jnp.moveaxis(edge, 2, 1)
    field = field + jnp.pad(edge, ((1, 0), (0, 0), (0, 0), (0, 96)))
    field = -0.25 * field
    return jnp.transpose(field, (1, 2, 0, 3)).reshape(owned, 8, width)


def solution(mesh):
    fine = Mesh(np.asarray(mesh.devices).reshape(8, 8, 2, 4), ("z", "y", "c", "x"))
    orb = ("z", "y", "c")
    return jax.shard_map(
        local,
        mesh=fine,
        in_specs=(
            P(orb, None, None),
            P(orb, "x", None),
            P(orb, "x", None),
            P(orb, "x", None),
        ),
        out_specs=P(orb, "x", None),
        check_vma=False,
    )
```
